8 devices in a mesh: dp: 1 (over z), tp: 8 (over x, y, core).
Axes of the slice: x: 2, y: 2, z: 1, core: 2. Of those that a mesh axis runs over, the one named last changes fastest.
Arguments:
- x: bfloat16 [2816, 3072], P(('dp', 'tp'))
- w_gate: bfloat16 [3072, 24576], P(None, 'tp')
- w_up: bfloat16 [3072, 24576], P(None, 'tp')
- w_down: bfloat16 [24576, 3072], P('tp')
Outputs:
- output: bfloat16 [2816, 3072], P(('dp', 'tp'))
All inputs are finite; a program needn't handle non-finite values.
Results may differ from the reference program's by a relative error of at most 0.016.
Values are sent between devices in bfloat16 or wider.
A program may use at most 2 GiB of HBM per device.

```python
import jax
import jax.numpy as jnp

ROWS = 2816
D = 3072
FF = 24576


def setup_inputs(seed: int = 0, part: int = 0) -> dict:
    kx, kg, ku, kd = jax.random.split(jax.random.key(seed), 4)
    drawn = {
        "x": jax.random.normal(jax.random.fold_in(kx, part), (ROWS, D), jnp.float32),
        "w_gate": jax.random.normal(kg, (D, FF), jnp.float32) * D**-0.5,
        "w_up": jax.random.normal(ku, (D, FF), jnp.float32) * D**-0.5,
        "w_down": jax.random.normal(kd, (FF, D), jnp.float32) * FF**-0.5,
    }
    return {k: v.astype(jnp.bfloat16) for k, v in drawn.items()}


def reference(x, w_gate, w_up, w_down):
    gate = jnp.dot(x, w_gate, preferred_element_type=jnp.float32)
    up = jnp.dot(x, w_up, preferred_element_type=jnp.float32)
    hidden = (jax.nn.gelu(gate) * up).astype(jnp.bfloat16)
    return jnp.dot(hidden, w_down, preferred_element_type=jnp.float32).astype(jnp.bfloat16)
```

```python
import jax
import jax.numpy as jnp
from jax import lax
from jax.experimental import pallas as pl
from jax.experimental.pallas import tpu as pltpu
from jax.sharding import PartitionSpec as P

ROWS = 352
HALF = 176
D = 3072
FF = 3072
N1 = 256
N2 = 512
T1, T2 = FF // N1, D // N2
R1, R2 = 3, 3
SLOTS = 5
BF16, F32 = jnp.bfloat16, jnp.float32


def kernel(
    x_hbm, wg, wu, wd, y_hbm,
    xo, xp, xg, h, bg, bu, bd, acc, own, psend, precv, rbuf,
    s_x, s_g, s_u, s_d, s_y,
    ag_s, ag_r, fw_s, fw_r, ps_s, ps_r, rs_s, rs_r,
):
    dp = lax.axis_index("dp")
    me = lax.axis_index("tp")
    k, iy, ix = lax.rem(me, 2), lax.rem(me // 2, 2), me // 4
    partner = me + 1 - 2 * k
    ynbr = me + 2 - 4 * iy
    xnbr = me + 4 - 8 * ix
    dnbr = xnbr + 2 - 4 * iy

    def remote(src, dst, ss, rs, dev):
        return pltpu.make_async_remote_copy(
            src_ref=src, dst_ref=dst, send_sem=ss, recv_sem=rs,
            device_id=(dp, dev), device_id_type=pl.DeviceIdType.MESH,
        )

    def gu_copies(kk):
        t, r = lax.rem(kk, T1), lax.rem(kk, R1)
        cols = pl.ds(pl.multiple_of(t * N1, N1), N1)
        return (
            pltpu.make_async_copy(wg.at[:, cols], bg.at[r], s_g.at[r]),
            pltpu.make_async_copy(wu.at[:, cols], bu.at[r], s_u.at[r]),
        )

    def d_copy(kk):
        t, r = lax.rem(kk, T2), lax.rem(kk, R2)
        cols = pl.ds(pl.multiple_of(t * N2, N2), N2)
        return pltpu.make_async_copy(wd.at[:, cols], bd.at[r], s_d.at[r])

    top, bot = pl.ds(0, HALF), pl.ds(HALF, HALF)
    to_partner = lambda: remote(x_hbm, xp, ag_s.at[0], ag_r.at[0], partner)
    x_first = lambda: remote(x_hbm.at[top], xg.at[0, top], ag_s.at[1], ag_r.at[1], xnbr)
    y_first = lambda: remote(x_hbm.at[bot], xg.at[0, bot], ag_s.at[2], ag_r.at[2], ynbr)
    relay_y = lambda: remote(xg.at[0, top], xg.at[1, top], ag_s.at[3], ag_r.at[3], ynbr)
    relay_x = lambda: remote(xg.at[0, bot], xg.at[1, bot], ag_s.at[4], ag_r.at[4], xnbr)
    x_second = lambda: remote(x_hbm.at[bot], xg.at[2, top], ag_s.at[5], ag_r.at[5], xnbr)
    y_second = lambda: remote(x_hbm.at[top], xg.at[2, bot], ag_s.at[6], ag_r.at[6], ynbr)

    def forward(s):
        return remote(
            xg.at[s, pl.ds(0, ROWS)], xg.at[s, pl.ds(ROWS, ROWS)], fw_s.at[s], fw_r.at[s], partner
        )

    def to_core(par, n):
        return remote(psend.at[n], precv.at[par, n], ps_s.at[n], ps_r.at[par, n], partner)

    def to_owner(s, n, sub):
        dev = dnbr if s == 1 else (xnbr if sub == 0 else ynbr)
        row = HALF * (sub if s < 2 else 1 - sub)
        cols = pl.ds(pl.multiple_of(n * N2, N2), N2)
        return remote(
            xg.at[s, pl.ds(ROWS + HALF * sub, HALF), cols],
            rbuf.at[s, n, pl.ds(row, HALF)],
            rs_s.at[s, sub, n], rs_r.at[s, sub, n], dev,
        )

    def lag(s, n):
        par = lax.rem(s, 2)
        to_core(par, n).wait_recv()
        total = own[lax.rem(n, 3)] + precv[par, n].astype(F32)
        xg[s, pl.ds(ROWS, ROWS), pl.ds(pl.multiple_of(n * N2, N2), N2)] = total.astype(BF16)
        for ss in range(3):
            @pl.when(s == ss)
            def _():
                to_owner(ss, n, 0).start()
                to_owner(ss, n, 1).start()

    def phase1(si, x_ref, rows, hook):
        def step(t, _):
            kk = si * T1 + t
            r = lax.rem(kk, R1)
            for c in gu_copies(kk):
                c.wait()

            @pl.when(kk + R1 - 1 < SLOTS * T1)
            def _():
                for c in gu_copies(kk + R1 - 1):
                    c.start()

            hook(t)
            gate = jnp.dot(x_ref[...], bg[r], preferred_element_type=F32)
            up = jnp.dot(x_ref[...], bu[r], preferred_element_type=F32)
            cols = pl.ds(pl.multiple_of(t * N1, N1), N1)
            h[pl.ds(0, rows), cols] = (jax.nn.gelu(gate) * up).astype(BF16)
            return 0

        lax.fori_loop(0, T1, step, 0)

    def phase2(si, rows, before, after):
        def step(n, _):
            kk = si * T2 + n
            d_copy(kk).wait()

            @pl.when(kk + R2 - 1 < SLOTS * T2)
            def _():
                d_copy(kk + R2 - 1).start()

            before(n)
            p = jnp.dot(h[pl.ds(0, rows), :], bd[lax.rem(kk, R2)], preferred_element_type=F32)
            after(n, p)
            return 0

        lax.fori_loop(0, T2, step, 0)

    x_in = pltpu.make_async_copy(x_hbm, xo, s_x)
    x_in.start()
    for i in range(R1 - 1):
        for c in gu_copies(i):
            c.start()
    barrier = pltpu.get_barrier_semaphore()
    for dev in (partner, xnbr, ynbr, dnbr):
        pl.semaphore_signal(
            barrier, inc=1, device_id=(dp, dev), device_id_type=pl.DeviceIdType.MESH
        )
    pl.semaphore_wait(barrier, 4)
    x_first().start()
    y_first().start()
    to_partner().start()
    x_in.wait()

    def hook0(t):
        @pl.when(t == 0)
        def _():
            for i in range(R2 - 1):
                d_copy(i).start()

    phase1(0, xo, ROWS, hook0)

    def after0(n, p):
        acc[n] = p

    phase2(0, ROWS, lambda n: None, after0)

    x_first().wait_recv()
    y_first().wait_recv()
    forward(0).start()
    relay_y().start()
    relay_x().start()
    x_second().start()
    y_second().start()

    def big(s, _):
        forward(s).wait_recv()

        def hook(t):
            @pl.when((t == 1) & (s > 0))
            def _():
                lag(s - 1, T2 - 2)
                lag(s - 1, T2 - 1)

        phase1(s + 1, xg.at[s], 2 * ROWS, hook)

        @pl.when(s == 0)
        def _():
            relay_y().wait_recv()
            relay_x().wait_recv()
            forward(1).start()

        @pl.when(s == 1)
        def _():
            x_second().wait_recv()
            y_second().wait_recv()
            forward(2).start()

        def before(n):
            @pl.when(n >= 2)
            def _():
                lag(s, n - 2)

            @pl.when(s > 0)
            def _():
                to_core(0, n).wait_send()

        def after(n, p):
            own[lax.rem(n, 3)] = p[:ROWS]
            psend[n] = p[ROWS:].astype(BF16)
            to_core(lax.rem(s, 2), n).start()

        phase2(s + 1, 2 * ROWS, before, after)
        return 0

    lax.fori_loop(0, 3, big, 0)

    to_partner().wait_recv()

    def hook4(t):
        @pl.when(t == 1)
        def _():
            lag(2, T2 - 2)
            lag(2, T2 - 1)

    phase1(4, xp, ROWS, hook4)

    def y_copy(n):
        cols = pl.ds(pl.multiple_of(n * N2, N2), N2)
        return pltpu.make_async_copy(precv.at[1, n], y_hbm.at[:, cols], s_y.at[n])

    def final(n):
        for ss in range(3):
            for sub in range(2):
                to_owner(ss, n, sub).wait_recv()
        to_core(1, n).wait_recv()
        total = acc[n] + precv[1, n].astype(F32)
        for ss in range(3):
            total = total + rbuf[ss, n].astype(F32)
        precv[1, n] = total.astype(BF16)
        y_copy(n).start()

    def before4(n):
        @pl.when(n >= 2)
        def _():
            final(n - 2)

        to_core(1, n).wait_send()

    def after4(n, p):
        psend[n] = p.astype(BF16)
        to_core(1, n).start()

    phase2(4, ROWS, before4, after4)
    final(T2 - 2)
    final(T2 - 1)

    for c in (to_partner, x_first, y_first, relay_y, relay_x, x_second, y_second):
        c().wait_send()
    for s in range(3):
        forward(s).wait_send()

    def drain(n, _):
        to_core(1, n).wait_send()
        for s in range(3):
            for sub in range(2):
                to_owner(s, n, sub).wait_send()
        y_copy(n).wait()
        return 0

    lax.fori_loop(0, T2, drain, 0)


def solution(mesh):
    hbm = pl.BlockSpec(memory_space=pl.ANY)
    dma = pltpu.SemaphoreType.DMA

    def step(x, w_gate, w_up, w_down):
        return pl.pallas_call(
            kernel,
            out_shape=jax.ShapeDtypeStruct((ROWS, D), BF16),
            in_specs=[hbm] * 4,
            out_specs=hbm,
            scratch_shapes=[
                pltpu.VMEM((ROWS, D), BF16),
                pltpu.VMEM((ROWS, D), BF16),
                pltpu.VMEM((3, 2 * ROWS, D), BF16),
                pltpu.VMEM((2 * ROWS, FF), BF16),
                pltpu.VMEM((R1, D, N1), BF16),
                pltpu.VMEM((R1, D, N1), BF16),
                pltpu.VMEM((R2, FF, N2), BF16),
                pltpu.VMEM((T2, ROWS, N2), F32),
                pltpu.VMEM((3, ROWS, N2), F32),
                pltpu.VMEM((T2, ROWS, N2), BF16),
                pltpu.VMEM((2, T2, ROWS, N2), BF16),
                pltpu.VMEM((3, T2, ROWS, N2), BF16),
                dma, dma((R1,)), dma((R1,)), dma((R2,)), dma((T2,)),
                dma((7,)), dma((7,)), dma((3,)), dma((3,)),
                dma((T2,)), dma((2, T2)), dma((3, 2, T2)), dma((3, 2, T2)),
            ],
            compiler_params=pltpu.CompilerParams(
                collective_id=0, has_side_effects=True, vmem_limit_bytes=67043328
            ),
            cost_estimate=pl.CostEstimate(
                flops=6 * 8 * ROWS * D * FF, bytes_accessed=5 * 6 * D * FF, transcendentals=8 * ROWS * FF
            ),
            name="mlp",
        )(x, w_gate, w_up, w_down)

    return jax.shard_map(
        step,
        mesh=mesh,
        in_specs=(P(("dp", "tp"), None), P(None, "tp"), P(None, "tp"), P("tp", None)),
        out_specs=P(("dp", "tp"), None),
        check_vma=False,
    )
```

```python
import jax
import jax.numpy as jnp
from jax import lax
from jax.experimental import pallas as pl
from jax.experimental.pallas import tpu as pltpu
from jax.sharding import PartitionSpec as P

ROWS = 352
HALF = 176
D = 3072
FF = 3072
N1 = 256
N2 = 512
T1, T2 = FF // N1, D // N2
STEPS = T1 + T2
RING = 6
SLOTS = 5
BF16, F32 = jnp.bfloat16, jnp.float32


def kernel(
    x_hbm, wg, wu, wd, y_hbm,
    xo, xp, xg, h, w0, w1, acc, own, psend, precv, rbuf,
    s_x, s_w0, s_w1, s_y,
    ag_s, ag_r, fw_s, fw_r, ps_s, ps_r, rs_s, rs_r,
):
    dp = lax.axis_index("dp")
    me = lax.axis_index("tp")
    k, iy, ix = lax.rem(me, 2), lax.rem(me // 2, 2), me // 4
    partner = me + 1 - 2 * k
    ynbr = me + 2 - 4 * iy
    xnbr = me + 4 - 8 * ix

    def remote(src, dst, ss, rs, dev):
        return pltpu.make_async_remote_copy(
            src_ref=src, dst_ref=dst, send_sem=ss, recv_sem=rs,
            device_id=(dp, dev), device_id_type=pl.DeviceIdType.MESH,
        )

    def pair(src0, col0, src1, col1, r):
        return (
            pltpu.make_async_copy(
                src0.at[:, pl.ds(pl.multiple_of(col0, N1), N1)], w0.at[r], s_w0.at[r]
            ),
            pltpu.make_async_copy(
                src1.at[:, pl.ds(pl.multiple_of(col1, N1), N1)], w1.at[r], s_w1.at[r]
            ),
        )

    def load(k):
        i, r = lax.rem(k, STEPS), lax.rem(k, RING)

        @pl.when((k < SLOTS * STEPS) & (i < T1))
        def _():
            for c in pair(wg, i * N1, wu, i * N1, r):
                c.start()

        @pl.when((k < SLOTS * STEPS) & (i >= T1))
        def _():
            n = i - T1
            for c in pair(wd, n * N2, wd, n * N2 + N1, r):
                c.start()

    def arrived(k):
        for c in pair(wg, 0, wu, 0, lax.rem(k, RING)):
            c.wait()

    def hidden(k, t, x_rows, row):
        r = lax.rem(k, RING)
        gate = jnp.dot(x_rows[...], w0[r], preferred_element_type=F32)
        up = jnp.dot(x_rows[...], w1[r], preferred_element_type=F32)
        cols = pl.ds(pl.multiple_of(t * N1, N1), N1)
        h[pl.ds(row, ROWS), cols] = (jax.nn.gelu(gate) * up).astype(BF16)

    def terms(k, row, store):
        r = lax.rem(k, RING)
        rows = h.at[pl.ds(row, ROWS)]
        store(pl.ds(0, N1), jnp.dot(rows[...], w0[r], preferred_element_type=F32))
        store(pl.ds(N1, N1), jnp.dot(rows[...], w1[r], preferred_element_type=F32))

    top, bot = pl.ds(0, HALF), pl.ds(HALF, HALF)
    to_partner = lambda: remote(x_hbm, xp, ag_s.at[0], ag_r.at[0], partner)
    x_first = lambda: remote(x_hbm.at[top], xg.at[0, top], ag_s.at[1], ag_r.at[1], xnbr)
    y_first = lambda: remote(x_hbm.at[bot], xg.at[0, bot], ag_s.at[2], ag_r.at[2], ynbr)
    relay_y = lambda: remote(xg.at[0, top], xg.at[1, top], ag_s.at[3], ag_r.at[3], ynbr)
    relay_x = lambda: remote(xg.at[0, bot], xg.at[1, bot], ag_s.at[4], ag_r.at[4], xnbr)
    x_second = lambda: remote(x_hbm.at[bot], xg.at[2, top], ag_s.at[5], ag_r.at[5], xnbr)
    y_second = lambda: remote(x_hbm.at[top], xg.at[2, bot], ag_s.at[6], ag_r.at[6], ynbr)

    def forward(s):
        return remote(
            xg.at[s, pl.ds(0, ROWS)], xg.at[s, pl.ds(ROWS, ROWS)], fw_s.at[s], fw_r.at[s], partner
        )

    def to_core(par, n):
        return remote(psend.at[n], precv.at[par, n], ps_s.at[n], ps_r.at[par, n], partner)

    def to_owner(s, n, sub):
        dev = xnbr if sub == 0 else ynbr
        row = HALF * (sub if s == 0 else 1 - sub)
        cols = pl.ds(pl.multiple_of(n * N2, N2), N2)
        return remote(
            xg.at[s, pl.ds(ROWS + HALF * sub, HALF), cols],
            rbuf.at[s, n, pl.ds(row, HALF)],
            rs_s.at[s, sub, n], rs_r.at[s, sub, n], dev,
        )

    def lag(s, n):
        par = s % 2
        to_core(par, n).wait_recv()
        total = own[n] + precv[par, n].astype(F32)
        if s == 2:
            to_owner(1, n, 0).wait_recv()
            to_owner(1, n, 1).wait_recv()
            total = total + rbuf[1, n].astype(F32)
        xg[s, pl.ds(ROWS, ROWS), pl.ds(n * N2, N2)] = total.astype(BF16)
        to_owner(s, n, 0).start()
        to_owner(s, n, 1).start()

    def phase1_small(si, x_ref, hook):
        def step(i, _):
            k = si * STEPS + 2 * i
            arrived(k)
            arrived(k + 1)

            @pl.when(k > 0)
            def _():
                load(k + 4)
                load(k + 5)

            hook(i)
            for j in range(2):
                hidden(k + j, 2 * i + j, x_ref, 0)
            return 0

        lax.fori_loop(0, T1 // 2, step, 0)

    x_in = pltpu.make_async_copy(x_hbm, xo, s_x)
    x_in.start()
    for i in range(RING):
        load(i)
    barrier = pltpu.get_barrier_semaphore()
    for dev in (partner, xnbr, ynbr):
        pl.semaphore_signal(
            barrier, inc=1, device_id=(dp, dev), device_id_type=pl.DeviceIdType.MESH
        )
    pl.semaphore_wait(barrier, 3)
    x_first().start()
    y_first().start()
    to_partner().start()
    x_in.wait()

    phase1_small(0, xo, lambda i: None)

    def step0(i, _):
        k = T1 + 2 * i
        arrived(k)
        arrived(k + 1)
        load(k + 4)
        load(k + 5)
        for j in range(2):
            def keep(cols, value):
                acc[2 * i + j, :, cols] = value

            terms(k + j, 0, keep)
        return 0

    lax.fori_loop(0, T2 // 2, step0, 0)

    x_first().wait_recv()
    y_first().wait_recv()
    forward(0).start()
    relay_y().start()
    relay_x().start()
    x_second().start()
    y_second().start()

    def big(s, _):
        forward(s).wait_recv()

        def step1(g, _):
            k = (s + 1) * STEPS + 3 * g
            for j in range(3):
                arrived(k + j)

            @pl.when(g > 0)
            def _():
                load(k + 3)

            load(k + 4)
            load(k + 5)
            for ss in range(1, 3):
                @pl.when((g == 0) & (s == ss))
                def _():
                    lag(ss - 1, 2)
                    lag(ss - 1, 3)

                @pl.when((g == 1) & (s == ss))
                def _():
                    lag(ss - 1, 4)
                    lag(ss - 1, 5)

            for j in range(3):
                for row in (0, ROWS):
                    hidden(k + j, 3 * g + j, xg.at[s, pl.ds(row, ROWS)], row)
            return 0

        lax.fori_loop(0, T1 // 3, step1, 0)

        @pl.when(s == 0)
        def _():
            relay_y().wait_recv()
            relay_x().wait_recv()
            forward(1).start()

        @pl.when(s == 1)
        def _():
            x_second().wait_recv()
            y_second().wait_recv()
            forward(2).start()

        for g in range(3):
            k = (s + 1) * STEPS + T1 + 2 * g
            arrived(k)
            arrived(k + 1)
            if g == 0:
                load(k + 3)
            load(k + 4)
            load(k + 5)
            if g == 2:
                for ss in range(3):
                    @pl.when(s == ss)
                    def _():
                        lag(ss, 0)
                        lag(ss, 1)

            @pl.when(s > 0)
            def _():
                for j in range(2):
                    to_core(0, 2 * g + j).wait_send()

            for j in range(2):
                n = 2 * g + j

                def theirs(cols, value):
                    psend[n, :, cols] = value.astype(BF16)

                def mine(cols, value):
                    own[n, :, cols] = value

                terms(k + j, ROWS, theirs)
                terms(k + j, 0, mine)
            for j in range(2):
                to_core(lax.rem(s, 2), 2 * g + j).start()
        return 0

    lax.fori_loop(0, 3, big, 0)

    to_partner().wait_recv()

    def hook4(i):
        for ii in range(2):
            @pl.when(i == ii)
            def _():
                lag(2, 2 * ii + 2)
                lag(2, 2 * ii + 3)

    phase1_small(4, xp, hook4)

    def y_copy(n):
        cols = pl.ds(pl.multiple_of(n * N2, N2), N2)
        return pltpu.make_async_copy(precv.at[1, n], y_hbm.at[:, cols], s_y.at[n])

    def final(n):
        for ss in (0, 2):
            for sub in range(2):
                to_owner(ss, n, sub).wait_recv()
        to_core(1, n).wait_recv()
        total = acc[n] + precv[1, n].astype(F32)
        for ss in (0, 2):
            total = total + rbuf[ss, n].astype(F32)
        precv[1, n] = total.astype(BF16)
        y_copy(n).start()

    for g in range(3):
        k = 4 * STEPS + T1 + 2 * g
        arrived(k)
        arrived(k + 1)
        if g == 0:
            load(k + 4)
            load(k + 5)
        if g == 2:
            final(0)
            final(1)
        for j in range(2):
            to_core(1, 2 * g + j).wait_send()
        for j in range(2):
            n = 2 * g + j

            def give(cols, value):
                psend[n, :, cols] = value.astype(BF16)

            terms(k + j, 0, give)
        for j in range(2):
            to_core(1, 2 * g + j).start()
    for n in range(2, T2):
        final(n)

    for c in (to_partner, x_first, y_first, relay_y, relay_x, x_second, y_second):
        c().wait_send()
    for s in range(3):
        forward(s).wait_send()

    def drain(n, _):
        to_core(1, n).wait_send()
        for s in range(3):
            for sub in range(2):
                to_owner(s, n, sub).wait_send()
        y_copy(n).wait()
        return 0

    lax.fori_loop(0, T2, drain, 0)


def solution(mesh):
    hbm = pl.BlockSpec(memory_space=pl.ANY)
    dma = pltpu.SemaphoreType.DMA

    def step(x, w_gate, w_up, w_down):
        return pl.pallas_call(
            kernel,
            out_shape=jax.ShapeDtypeStruct((ROWS, D), BF16),
            in_specs=[hbm] * 4,
            out_specs=hbm,
            scratch_shapes=[
                pltpu.VMEM((ROWS, D), BF16),
                pltpu.VMEM((ROWS, D), BF16),
                pltpu.VMEM((3, 2 * ROWS, D), BF16),
                pltpu.VMEM((2 * ROWS, FF), BF16),
                pltpu.VMEM((RING, D, N1), BF16),
                pltpu.VMEM((RING, D, N1), BF16),
                pltpu.VMEM((T2, ROWS, N2), F32),
                pltpu.VMEM((T2, ROWS, N2), F32),
                pltpu.VMEM((T2, ROWS, N2), BF16),
                pltpu.VMEM((2, T2, ROWS, N2), BF16),
                pltpu.VMEM((3, T2, ROWS, N2), BF16),
                dma, dma((RING,)), dma((RING,)), dma((T2,)),
                dma((7,)), dma((7,)), dma((3,)), dma((3,)),
                dma((T2,)), dma((2, T2)), dma((3, 2, T2)), dma((3, 2, T2)),
            ],
            compiler_params=pltpu.CompilerParams(
                collective_id=0, has_side_effects=True, vmem_limit_bytes=67043328,
            ),
            cost_estimate=pl.CostEstimate(
                flops=6 * 8 * ROWS * D * FF, bytes_accessed=5 * 6 * D * FF, transcendentals=8 * ROWS * FF
            ),
            name="mlp",
        )(x, w_gate, w_up, w_down)

    return jax.shard_map(
        step,
        mesh=mesh,
        in_specs=(P(("dp", "tp"), None), P(None, "tp"), P(None, "tp"), P("tp", None)),
        out_specs=P(("dp", "tp"), None),
        check_vma=False,
    )
```

```python
import jax
import jax.numpy as jnp
from jax import lax
from jax.experimental import pallas as pl
from jax.experimental.pallas import tpu as pltpu
from jax.sharding import PartitionSpec as P

ROWS = 352
HALF = 176
D = 3072
FF = 3072
N1 = 256
N2 = 512
T1, T2 = FF // N1, D // N2
STEPS = T1 + T2
RING = 6
SLOTS = 5
BF16, F32 = jnp.bfloat16, jnp.float32


def kernel(
    x_hbm, wg, wu, wd, y_hbm,
    xo, xp, xg, h, w0, w1, acc, own, psend, precv, rbuf,
    s_x, s_w0, s_w1, s_y,
    ag_s, ag_r, fw_s, fw_r, ps_s, ps_r, rs_s, rs_r,
):
    dp = lax.axis_index("dp")
    me = lax.axis_index("tp")
    k, iy, ix = lax.rem(me, 2), lax.rem(me // 2, 2), me // 4
    partner = me + 1 - 2 * k
    ynbr = me + 2 - 4 * iy
    xnbr = me + 4 - 8 * ix

    def remote(src, dst, ss, rs, dev):
        return pltpu.make_async_remote_copy(
            src_ref=src, dst_ref=dst, send_sem=ss, recv_sem=rs,
            device_id=(dp, dev), device_id_type=pl.DeviceIdType.MESH,
        )

    def pair(src0, col0, src1, col1, r):
        return (
            pltpu.make_async_copy(
                src0.at[:, pl.ds(pl.multiple_of(col0, N1), N1)], w0.at[r], s_w0.at[r]
            ),
            pltpu.make_async_copy(
                src1.at[:, pl.ds(pl.multiple_of(col1, N1), N1)], w1.at[r], s_w1.at[r]
            ),
        )

    def load(k):
        i, r = lax.rem(k, STEPS), lax.rem(k, RING)

        @pl.when((k < SLOTS * STEPS) & (i < T1))
        def _():
            for c in pair(wg, i * N1, wu, i * N1, r):
                c.start()

        @pl.when((k < SLOTS * STEPS) & (i >= T1))
        def _():
            n = i - T1
            for c in pair(wd, n * N2, wd, n * N2 + N1, r):
                c.start()

    def arrived(k):
        for c in pair(wg, 0, wu, 0, lax.rem(k, RING)):
            c.wait()

    def hidden(k, t, x_rows, row):
        r = lax.rem(k, RING)
        gate = jnp.dot(x_rows[...], w0[r], preferred_element_type=F32)
        up = jnp.dot(x_rows[...], w1[r], preferred_element_type=F32)
        cols = pl.ds(pl.multiple_of(t * N1, N1), N1)
        h[pl.ds(row, ROWS), cols] = (jax.nn.gelu(gate) * up).astype(BF16)

    def terms(k, row, store):
        r = lax.rem(k, RING)
        rows = h.at[pl.ds(row, ROWS)]
        store(pl.ds(0, N1), jnp.dot(rows[...], w0[r], preferred_element_type=F32))
        store(pl.ds(N1, N1), jnp.dot(rows[...], w1[r], preferred_element_type=F32))

    upper, lower = pl.ds(0, HALF), pl.ds(HALF, HALF)
    parts = ((0, 64), (64, 64), (128, HALF - 128))
    to_partner = lambda: remote(x_hbm, xp, ag_s.at[0], ag_r.at[0], partner)

    def first(sub, part):
        rows = pl.ds(HALF * sub + parts[part][0], parts[part][1])
        return remote(
            x_hbm.at[rows], xg.at[0, rows],
            ag_s.at[5 + 3 * sub + part], ag_r.at[5 + 3 * sub + part], ynbr if sub else xnbr,
        )

    relay_y = lambda: remote(xg.at[0, upper], xg.at[1, upper], ag_s.at[3], ag_r.at[3], ynbr)
    relay_x = lambda: remote(xg.at[0, lower], xg.at[1, lower], ag_s.at[4], ag_r.at[4], xnbr)
    x_second = lambda: remote(x_hbm.at[lower], xg.at[2, upper], ag_s.at[1], ag_r.at[1], xnbr)
    y_second = lambda: remote(x_hbm.at[upper], xg.at[2, lower], ag_s.at[2], ag_r.at[2], ynbr)

    def forward_first(sub, part):
        row, n = HALF * sub + parts[part][0], parts[part][1]
        return remote(
            xg.at[0, pl.ds(row, n)], xg.at[0, pl.ds(ROWS + row, n)],
            fw_s.at[3 * sub + part], fw_r.at[3 * sub + part], partner,
        )

    def forward(s):
        return remote(
            xg.at[s, pl.ds(0, ROWS)], xg.at[s, pl.ds(ROWS, ROWS)], fw_s.at[5 + s], fw_r.at[5 + s], partner
        )

    def to_core(par, n):
        return remote(psend.at[n], precv.at[par, n], ps_s.at[n], ps_r.at[par, n], partner)

    def to_owner(s, n, sub):
        dev = xnbr if sub == 0 else ynbr
        row = HALF * (sub if s == 0 else 1 - sub)
        cols = pl.ds(pl.multiple_of(n * N2, N2), N2)
        return remote(
            xg.at[s, pl.ds(ROWS + HALF * sub, HALF), cols],
            rbuf.at[s, n, pl.ds(row, HALF)],
            rs_s.at[s, sub, n], rs_r.at[s, sub, n], dev,
        )

    def lag(s, n):
        par = s % 2
        to_core(par, n).wait_recv()
        total = own[n] + precv[par, n].astype(F32)
        if s == 2:
            to_owner(1, n, 0).wait_recv()
            to_owner(1, n, 1).wait_recv()
            total = total + rbuf[1, n].astype(F32)
        xg[s, pl.ds(ROWS, ROWS), pl.ds(n * N2, N2)] = total.astype(BF16)
        to_owner(s, n, 0).start()
        to_owner(s, n, 1).start()

    def phase1_small(si, x_ref, hook):
        def step(i, _):
            k = si * STEPS + 3 * i
            for j in range(3):
                arrived(k + j)

            @pl.when(i > 0)
            def _():
                load(k + 3)

            @pl.when(k > 0)
            def _():
                load(k + 4)
                load(k + 5)

            hook(i)
            for j in range(3):
                hidden(k + j, 3 * i + j, x_ref, 0)
            return 0

        lax.fori_loop(0, T1 // 3, step, 0)

    x_in = pltpu.make_async_copy(x_hbm, xo, s_x)
    x_in.start()
    for i in range(RING):
        load(i)
    barrier = pltpu.get_barrier_semaphore()
    for dev in (partner, xnbr, ynbr):
        pl.semaphore_signal(
            barrier, inc=1, device_id=(dp, dev), device_id_type=pl.DeviceIdType.MESH
        )
    pl.semaphore_wait(barrier, 3)
    for part in range(3):
        for sub in range(2):
            first(sub, part).start()
    to_partner().start()
    x_in.wait()

    phase1_small(0, xo, lambda i: None)

    def step0(i, _):
        k = T1 + 3 * i
        for j in range(3):
            arrived(k + j)
        for j in range(3):
            load(k + 3 + j)

        @pl.when(i == 1)
        def _():
            for part in range(2):
                for sub in range(2):
                    first(sub, part).wait_recv()
                    forward_first(sub, part).start()

        for j in range(3):
            def keep(cols, value):
                acc[3 * i + j, :, cols] = value

            terms(k + j, 0, keep)
        return 0

    lax.fori_loop(0, T2 // 3, step0, 0)

    for sub in range(2):
        first(sub, 2).wait_recv()
        forward_first(sub, 2).start()
    relay_y().start()
    relay_x().start()
    x_second().start()
    y_second().start()
    for part in range(3):
        for sub in range(2):
            forward_first(sub, part).wait_recv()

    def big(s, _):
        @pl.when(s == 1)
        def _():
            forward(1).wait_recv()

        @pl.when(s == 2)
        def _():
            forward(2).wait_recv()

        def step1(g, _):
            k = (s + 1) * STEPS + 3 * g
            for j in range(3):
                arrived(k + j)

            @pl.when((g > 0) | (s == 0))
            def _():
                load(k + 3)

            load(k + 4)
            load(k + 5)
            for ss in range(1, 3):
                @pl.when((g == 0) & (s == ss))
                def _():
                    lag(ss - 1, 2)
                    lag(ss - 1, 3)

                @pl.when((g == 1) & (s == ss))
                def _():
                    lag(ss - 1, 4)
                    lag(ss - 1, 5)

            for j in range(3):
                for row in (0, ROWS):
                    hidden(k + j, 3 * g + j, xg.at[s, pl.ds(row, ROWS)], row)
            return 0

        lax.fori_loop(0, T1 // 3, step1, 0)

        @pl.when(s == 0)
        def _():
            relay_y().wait_recv()
            relay_x().wait_recv()
            forward(1).start()

        @pl.when(s == 1)
        def _():
            x_second().wait_recv()
            y_second().wait_recv()
            forward(2).start()

        for g in range(3):
            k = (s + 1) * STEPS + T1 + 2 * g
            arrived(k)
            arrived(k + 1)
            if g == 0:
                load(k + 3)
            load(k + 4)
            load(k + 5)
            if g == 2:
                for ss in range(3):
                    @pl.when(s == ss)
                    def _():
                        lag(ss, 0)
                        lag(ss, 1)

            @pl.when(s > 0)
            def _():
                for j in range(2):
                    to_core(0, 2 * g + j).wait_send()

            for j in range(2):
                n = 2 * g + j

                def theirs(cols, value):
                    psend[n, :, cols] = value.astype(BF16)

                def mine(cols, value):
                    own[n, :, cols] = value

                terms(k + j, ROWS, theirs)
                terms(k + j, 0, mine)
            for j in range(2):
                to_core(lax.rem(s, 2), 2 * g + j).start()
        return 0

    lax.fori_loop(0, 3, big, 0)

    to_partner().wait_recv()

    def hook4(i):
        for ii in range(2):
            @pl.when(i == ii)
            def _():
                lag(2, 2 * ii + 2)
                lag(2, 2 * ii + 3)

    phase1_small(4, xp, hook4)

    def y_copy(n):
        cols = pl.ds(pl.multiple_of(n * N2, N2), N2)
        return pltpu.make_async_copy(precv.at[1, n], y_hbm.at[:, cols], s_y.at[n])

    def final(n):
        for ss in (0, 2):
            for sub in range(2):
                to_owner(ss, n, sub).wait_recv()
        to_core(1, n).wait_recv()
        total = acc[n] + precv[1, n].astype(F32)
        for ss in (0, 2):
            total = total + rbuf[ss, n].astype(F32)
        precv[1, n] = total.astype(BF16)
        y_copy(n).start()

    for g in range(3):
        k = 4 * STEPS + T1 + 2 * g
        arrived(k)
        arrived(k + 1)
        if g == 0:
            for j in range(3, 6):
                load(k + j)
        if g == 2:
            final(0)
            final(1)
        for j in range(2):
            to_core(1, 2 * g + j).wait_send()
        for j in range(2):
            n = 2 * g + j

            def give(cols, value):
                psend[n, :, cols] = value.astype(BF16)

            terms(k + j, 0, give)
        for j in range(2):
            to_core(1, 2 * g + j).start()
    for n in range(2, T2):
        final(n)

    for c in (to_partner, relay_y, relay_x, x_second, y_second):
        c().wait_send()
    for part in range(3):
        for sub in range(2):
            first(sub, part).wait_send()
            forward_first(sub, part).wait_send()
    for s in (1, 2):
        forward(s).wait_send()

    def drain(n, _):
        to_core(1, n).wait_send()
        for s in range(3):
            for sub in range(2):
                to_owner(s, n, sub).wait_send()
        y_copy(n).wait()
        return 0

    lax.fori_loop(0, T2, drain, 0)


def solution(mesh):
    hbm = pl.BlockSpec(memory_space=pl.ANY)
    dma = pltpu.SemaphoreType.DMA

    def step(x, w_gate, w_up, w_down):
        return pl.pallas_call(
            kernel,
            out_shape=jax.ShapeDtypeStruct((ROWS, D), BF16),
            in_specs=[hbm] * 4,
            out_specs=hbm,
            scratch_shapes=[
                pltpu.VMEM((ROWS, D), BF16),
                pltpu.VMEM((ROWS, D), BF16),
                pltpu.VMEM((3, 2 * ROWS, D), BF16),
                pltpu.VMEM((2 * ROWS, FF), BF16),
                pltpu.VMEM((RING, D, N1), BF16),
                pltpu.VMEM((RING, D, N1), BF16),
                pltpu.VMEM((T2, ROWS, N2), F32),
                pltpu.VMEM((T2, ROWS, N2), F32),
                pltpu.VMEM((T2, ROWS, N2), BF16),
                pltpu.VMEM((2, T2, ROWS, N2), BF16),
                pltpu.VMEM((3, T2, ROWS, N2), BF16),
                dma, dma((RING,)), dma((RING,)), dma((T2,)),
                dma((11,)), dma((11,)), dma((8,)), dma((8,)),
                dma((T2,)), dma((2, T2)), dma((3, 2, T2)), dma((3, 2, T2)),
            ],
            compiler_params=pltpu.CompilerParams(
                collective_id=0, has_side_effects=True, vmem_limit_bytes=67043328,
            ),
            cost_estimate=pl.CostEstimate(
                flops=6 * 8 * ROWS * D * FF, bytes_accessed=5 * 6 * D * FF, transcendentals=8 * ROWS * FF
            ),
            name="mlp",
        )(x, w_gate, w_up, w_down)

    return jax.shard_map(
        step,
        mesh=mesh,
        in_specs=(P(("dp", "tp"), None), P(None, "tp"), P(None, "tp"), P("tp", None)),
        out_specs=P(("dp", "tp"), None),
        check_vma=False,
    )
```

```python
import jax
import jax.numpy as jnp
from jax import lax
from jax.experimental import pallas as pl
from jax.experimental.pallas import tpu as pltpu
from jax.sharding import PartitionSpec as P

ROWS = 352
HALF = 176
D = 3072
FF = 3072
N1 = 256
N2 = 512
T1, T2 = FF // N1, D // N2
STEPS = T1 + T2
RING = 6
SLOTS = 5
BF16, F32 = jnp.bfloat16, jnp.float32


def kernel(
    x_hbm, wg, wu, wd, y_hbm,
    xo, xp, xg, h, w0, w1, acc, own, psend, precv, rbuf,
    s_x, s_w0, s_w1, s_y,
    ag_s, ag_r, fw_s, fw_r, ps_s, ps_r, rs_s, rs_r,
):
    dp = lax.axis_index("dp")
    me = lax.axis_index("tp")
    k, iy, ix = lax.rem(me, 2), lax.rem(me // 2, 2), me // 4
    partner = me + 1 - 2 * k
    ynbr = me + 2 - 4 * iy
    xnbr = me + 4 - 8 * ix

    def remote(src, dst, ss, rs, dev):
        return pltpu.make_async_remote_copy(
            src_ref=src, dst_ref=dst, send_sem=ss, recv_sem=rs,
            device_id=(dp, dev), device_id_type=pl.DeviceIdType.MESH,
        )

    def pair(src0, col0, src1, col1, r):
        return (
            pltpu.make_async_copy(
                src0.at[:, pl.ds(pl.multiple_of(col0, N1), N1)], w0.at[r], s_w0.at[r]
            ),
            pltpu.make_async_copy(
                src1.at[:, pl.ds(pl.multiple_of(col1, N1), N1)], w1.at[r], s_w1.at[r]
            ),
        )

    def load(k):
        i, r = lax.rem(k, STEPS), lax.rem(k, RING)

        @pl.when((k < SLOTS * STEPS) & (i < T1))
        def _():
            for c in pair(wg, i * N1, wu, i * N1, r):
                c.start()

        @pl.when((k < SLOTS * STEPS) & (i >= T1))
        def _():
            n = i - T1
            for c in pair(wd, n * N2, wd, n * N2 + N1, r):
                c.start()

    def arrived(k):
        for c in pair(wg, 0, wu, 0, lax.rem(k, RING)):
            c.wait()

    def hidden(k, t, x_rows, row):
        r = lax.rem(k, RING)
        gate = jnp.dot(x_rows[...], w0[r], preferred_element_type=F32)
        up = jnp.dot(x_rows[...], w1[r], preferred_element_type=F32)
        cols = pl.ds(pl.multiple_of(t * N1, N1), N1)
        h[pl.ds(row, ROWS), cols] = (jax.nn.gelu(gate) * up).astype(BF16)

    def terms(k, row, store):
        r = lax.rem(k, RING)
        rows = h.at[pl.ds(row, ROWS)]
        store(pl.ds(0, N1), jnp.dot(rows[...], w0[r], preferred_element_type=F32))
        store(pl.ds(N1, N1), jnp.dot(rows[...], w1[r], preferred_element_type=F32))

    upper, lower = pl.ds(0, HALF), pl.ds(HALF, HALF)
    parts = ((0, 64), (64, 64), (128, HALF - 128))
    to_partner = lambda: remote(x_hbm, xp, ag_s.at[0], ag_r.at[0], partner)

    def first(sub, part):
        rows = pl.ds(HALF * sub + parts[part][0], parts[part][1])
        return remote(
            x_hbm.at[rows], xg.at[0, rows],
            ag_s.at[5 + 3 * sub + part], ag_r.at[5 + 3 * sub + part], ynbr if sub else xnbr,
        )

    relay_y = lambda: remote(xg.at[0, upper], xg.at[1, upper], ag_s.at[3], ag_r.at[3], ynbr)
    relay_x = lambda: remote(xg.at[0, lower], xg.at[1, lower], ag_s.at[4], ag_r.at[4], xnbr)
    x_second = lambda: remote(x_hbm.at[lower], xg.at[2, upper], ag_s.at[1], ag_r.at[1], xnbr)
    y_second = lambda: remote(x_hbm.at[upper], xg.at[2, lower], ag_s.at[2], ag_r.at[2], ynbr)

    def forward_first(sub, part):
        row, n = HALF * sub + parts[part][0], parts[part][1]
        return remote(
            xg.at[0, pl.ds(row, n)], xg.at[0, pl.ds(ROWS + row, n)],
            fw_s.at[3 * sub + part], fw_r.at[3 * sub + part], partner,
        )

    def forward(s):
        return remote(
            xg.at[s, pl.ds(0, ROWS)], xg.at[s, pl.ds(ROWS, ROWS)], fw_s.at[5 + s], fw_r.at[5 + s], partner
        )

    def to_core(par, n):
        return remote(psend.at[n], precv.at[par, n], ps_s.at[n], ps_r.at[par, n], partner)

    def to_owner(s, n, sub):
        dev = xnbr if sub == 0 else ynbr
        row = HALF * (sub if s == 0 else 1 - sub)
        cols = pl.ds(pl.multiple_of(n * N2, N2), N2)
        return remote(
            xg.at[s, pl.ds(ROWS + HALF * sub, HALF), cols],
            rbuf.at[s, n, pl.ds(row, HALF)],
            rs_s.at[s, sub, n], rs_r.at[s, sub, n], dev,
        )

    def lag(s, n):
        par = s % 2
        to_core(par, n).wait_recv()
        total = own[n] + precv[par, n].astype(F32)
        if s == 2:
            to_owner(1, n, 0).wait_recv()
            to_owner(1, n, 1).wait_recv()
            total = total + rbuf[1, n].astype(F32)
        xg[s, pl.ds(ROWS, ROWS), pl.ds(n * N2, N2)] = total.astype(BF16)
        to_owner(s, n, 0).start()
        to_owner(s, n, 1).start()

    def phase1_small(si, x_ref, hook):
        def step(i, _):
            k = si * STEPS + 3 * i
            for j in range(3):
                arrived(k + j)

            @pl.when(k > 0)
            def _():
                for j in range(3, 6):
                    load(k + j)

            hook(i)
            for j in range(3):
                hidden(k + j, 3 * i + j, x_ref, 0)
            return 0

        lax.fori_loop(0, T1 // 3, step, 0)

    x_in = pltpu.make_async_copy(x_hbm, xo, s_x)
    x_in.start()
    for i in range(RING):
        load(i)
    barrier = pltpu.get_barrier_semaphore()
    for dev in (partner, xnbr, ynbr):
        pl.semaphore_signal(
            barrier, inc=1, device_id=(dp, dev), device_id_type=pl.DeviceIdType.MESH
        )
    pl.semaphore_wait(barrier, 3)
    for part in range(3):
        for sub in range(2):
            first(sub, part).start()
    to_partner().start()
    x_in.wait()

    phase1_small(0, xo, lambda i: None)

    def step0(i, _):
        k = T1 + 3 * i
        for j in range(3):
            arrived(k + j)
        for j in range(3):
            load(k + 3 + j)

        @pl.when(i == 1)
        def _():
            for part in range(2):
                for sub in range(2):
                    first(sub, part).wait_recv()
                    forward_first(sub, part).start()

        for j in range(3):
            def keep(cols, value):
                acc[3 * i + j, :, cols] = value

            terms(k + j, 0, keep)
        return 0

    lax.fori_loop(0, T2 // 3, step0, 0)

    for sub in range(2):
        first(sub, 2).wait_recv()
        forward_first(sub, 2).start()
    relay_y().start()
    relay_x().start()
    x_second().start()
    y_second().start()
    for part in range(3):
        for sub in range(2):
            forward_first(sub, part).wait_recv()

    def big(s, _):
        @pl.when(s == 1)
        def _():
            forward(1).wait_recv()

        @pl.when(s == 2)
        def _():
            forward(2).wait_recv()

        def step1(g, _):
            k = (s + 1) * STEPS + 3 * g
            for j in range(3):
                arrived(k + j)

            for j in range(3, 6):
                load(k + j)
            for ss in range(1, 3):
                @pl.when((g == 0) & (s == ss))
                def _():
                    for n in range(3):
                        lag(ss - 1, n)

                @pl.when((g == 1) & (s == ss))
                def _():
                    for n in range(3, 6):
                        lag(ss - 1, n)

            for j in range(3):
                for row in (0, ROWS):
                    hidden(k + j, 3 * g + j, xg.at[s, pl.ds(row, ROWS)], row)
            return 0

        lax.fori_loop(0, T1 // 3, step1, 0)

        @pl.when(s == 0)
        def _():
            relay_y().wait_recv()
            relay_x().wait_recv()
            forward(1).start()

        @pl.when(s == 1)
        def _():
            x_second().wait_recv()
            y_second().wait_recv()
            forward(2).start()

        for g in range(2):
            k = (s + 1) * STEPS + T1 + 3 * g
            for j in range(3):
                arrived(k + j)
            for j in range(3, 6):
                load(k + j)

            @pl.when(s > 0)
            def _():
                for j in range(3):
                    to_core(0, 3 * g + j).wait_send()

            for j in range(3):
                n = 3 * g + j

                def theirs(cols, value):
                    psend[n, :, cols] = value.astype(BF16)

                def mine(cols, value):
                    own[n, :, cols] = value

                terms(k + j, ROWS, theirs)
                terms(k + j, 0, mine)
            for j in range(3):
                to_core(lax.rem(s, 2), 3 * g + j).start()
        return 0

    lax.fori_loop(0, 3, big, 0)

    to_partner().wait_recv()

    def hook4(i):
        for ii in range(2):
            @pl.when(i == ii)
            def _():
                for n in range(3 * ii, 3 * ii + 3):
                    lag(2, n)

    phase1_small(4, xp, hook4)

    def y_copy(n):
        cols = pl.ds(pl.multiple_of(n * N2, N2), N2)
        return pltpu.make_async_copy(precv.at[1, n], y_hbm.at[:, cols], s_y.at[n])

    def final(n):
        for ss in (0, 2):
            for sub in range(2):
                to_owner(ss, n, sub).wait_recv()
        to_core(1, n).wait_recv()
        total = acc[n] + precv[1, n].astype(F32)
        for ss in (0, 2):
            total = total + rbuf[ss, n].astype(F32)
        precv[1, n] = total.astype(BF16)
        y_copy(n).start()

    for g in range(3):
        k = 4 * STEPS + T1 + 2 * g
        arrived(k)
        arrived(k + 1)
        if g == 0:
            for j in range(3, 6):
                load(k + j)
        if g == 2:
            final(0)
            final(1)
        for j in range(2):
            to_core(1, 2 * g + j).wait_send()
        for j in range(2):
            n = 2 * g + j

            def give(cols, value):
                psend[n, :, cols] = value.astype(BF16)

            terms(k + j, 0, give)
        for j in range(2):
            to_core(1, 2 * g + j).start()
    for n in range(2, T2):
        final(n)

    for c in (to_partner, relay_y, relay_x, x_second, y_second):
        c().wait_send()
    for part in range(3):
        for sub in range(2):
            first(sub, part).wait_send()
            forward_first(sub, part).wait_send()
    for s in (1, 2):
        forward(s).wait_send()

    def drain(n, _):
        to_core(1, n).wait_send()
        for s in range(3):
            for sub in range(2):
                to_owner(s, n, sub).wait_send()
        y_copy(n).wait()
        return 0

    lax.fori_loop(0, T2, drain, 0)


def solution(mesh):
    hbm = pl.BlockSpec(memory_space=pl.ANY)
    dma = pltpu.SemaphoreType.DMA

    def step(x, w_gate, w_up, w_down):
        return pl.pallas_call(
            kernel,
            out_shape=jax.ShapeDtypeStruct((ROWS, D), BF16),
            in_specs=[hbm] * 4,
            out_specs=hbm,
            scratch_shapes=[
                pltpu.VMEM((ROWS, D), BF16),
                pltpu.VMEM((ROWS, D), BF16),
                pltpu.VMEM((3, 2 * ROWS, D), BF16),
                pltpu.VMEM((2 * ROWS, FF), BF16),
                pltpu.VMEM((RING, D, N1), BF16),
                pltpu.VMEM((RING, D, N1), BF16),
                pltpu.VMEM((T2, ROWS, N2), F32),
                pltpu.VMEM((T2, ROWS, N2), F32),
                pltpu.VMEM((T2, ROWS, N2), BF16),
                pltpu.VMEM((2, T2, ROWS, N2), BF16),
                pltpu.VMEM((3, T2, ROWS, N2), BF16),
                dma, dma((RING,)), dma((RING,)), dma((T2,)),
                dma((11,)), dma((11,)), dma((8,)), dma((8,)),
                dma((T2,)), dma((2, T2)), dma((3, 2, T2)), dma((3, 2, T2)),
            ],
            compiler_params=pltpu.CompilerParams(
                collective_id=0, has_side_effects=True, vmem_limit_bytes=67043328,
            ),
            cost_estimate=pl.CostEstimate(
                flops=6 * 8 * ROWS * D * FF, bytes_accessed=5 * 6 * D * FF, transcendentals=8 * ROWS * FF
            ),
            name="mlp",
        )(x, w_gate, w_up, w_down)

    return jax.shard_map(
        step,
        mesh=mesh,
        in_specs=(P(("dp", "tp"), None), P(None, "tp"), P(None, "tp"), P("tp", None)),
        out_specs=P(("dp", "tp"), None),
        check_vma=False,
    )
```
